32 devices in a mesh: ka: 8 (over y, x, core), ga: 4 (over z).
Axes of the slice: x: 2, y: 2, z: 4, core: 2. Of those that a mesh axis runs over, the one named last changes fastest.
Arguments:
- coeffs: bfloat16 [8, 2, 7680, 256], P('ka', None, 'ga'), may hold values from -1 to 1
- projectors: bfloat16 [2, 7680, 1024], P(None, 'ga'), may hold values from -1.5 to 1.5
- proj_deriv: bfloat16 [2, 7680, 1024], P(None, 'ga'), may hold values from -1.5 to 1.5
- shift_map: int32 [7680], P('ga'), may hold values from 0 to 7679, as said below
- atom_of: int32 [1024], replicated, may hold values from 0 to 127, as said below
Outputs:
- transport: float32 [8, 2, 256, 256], P('ka')
- forces: float32 [128], replicated
The draws below stay inside these ranges and needn't reach their ends.
Inputs may be any that keep to these rules, and one draw needn't show every extreme that they name: `shift_map`: a permutation that maps each aligned block of 1920 plane waves onto itself. `atom_of`: each atom owns exactly 8 projectors.
All inputs are finite; a program needn't handle non-finite values.
Results may differ from the reference program's by a relative error of at most 0.0003.
Values may be sent and summed in bfloat16 or wider, within the bound.
No kernel may reach another device: no remote copies, remote signals or barrier semaphores. Data moves between devices by JAX's collectives and lax.ppermute only.
A program may use at most 128 MiB of HBM per device.

```python
import math
import jax
import jax.numpy as jnp
from jax import lax

NB = 256
GD = 1920
NP = 1024
NA = 128
NEWTON = 2
NK = 8
NG = 7680


def block_shift(key):
    start_key = jax.random.fold_in(key, 11)
    block_keys = jax.random.split(start_key, NG // GD)
    shuffled = jax.vmap(lambda single: jax.random.permutation(single, GD))(block_keys)
    offsets = jnp.arange(NG // GD, dtype=jnp.int32) * GD
    return (shuffled.astype(jnp.int32) + offsets[:, None]).reshape(NG)


def draw_shift_map(key, part):
    return block_shift(key)


def draw_coeffs(key, part):
    mapping = block_shift(key)
    common_key = jax.random.fold_in(key, 21)
    spread_key = jax.random.fold_in(key, 22)
    common = jax.random.normal(common_key, (2, NG, NB), jnp.float32)
    spread_part = 0.3 * jax.random.normal(spread_key, (NK, 2, NG, NB), jnp.float32)
    norming = (2.0 * NG) ** (-0.5)
    common = common * norming
    spread_part = spread_part * norming
    angles = math.pi / 2 * jnp.arange(NK, dtype=jnp.float32) / NK
    moved = common[:, mapping, :]
    values = jnp.cos(angles)[:, None, None, None] * common[None] + jnp.sin(angles)[:, None, None, None] * moved[None] + spread_part
    return jnp.clip(values, -1.0, 1.0).astype(jnp.bfloat16)


def draw_atom_of(key, part):
    order = jax.random.permutation(jax.random.fold_in(key, 31), NP)
    return (order // (NP // NA)).astype(jnp.int32)


def level_of(stream_key, extent, pieces, smallest, top_value):
    def one(dim, parts):
        heights = jax.random.uniform(jax.random.fold_in(jax.random.fold_in(stream_key, 6), dim), (parts,), jnp.float32, smallest / len(pieces), top_value / len(pieces))
        return jnp.repeat(jnp.exp(heights), extent[dim] // parts).reshape((-1,) + (1,) * (len(extent) - dim - 1))

    factor_of = one(*pieces[0])
    for cut in pieces[1:]:
        factor_of = factor_of * one(*cut)
    return factor_of


def gaussian(stream_key, extent, scale, bound, pieces=(), kind=jnp.bfloat16):
    drawn = jax.random.normal(stream_key, extent, jnp.float32) * scale
    if len(pieces) > 0:
        drawn = level_of(stream_key, extent, pieces, -0.22, 0.18) * drawn
    return jnp.clip(drawn, min=-bound, max=bound).astype(kind)


def setup_inputs(seed: int = 0) -> dict:
    arg_keys = jax.random.split(jax.random.key(seed), 6)
    return {
        "coeffs": draw_coeffs(jax.random.fold_in(arg_keys[5], 71), 0),
        "projectors": gaussian(arg_keys[1], (2, NG, NP), 0.25, 1.5, ((1, 4),)),
        "proj_deriv": gaussian(arg_keys[2], (2, NG, NP), 0.25, 1.5, ((1, 4),)),
        "shift_map": draw_shift_map(jax.random.fold_in(arg_keys[5], 71), 0),
        "atom_of": draw_atom_of(jax.random.fold_in(arg_keys[5], 71), 0),
    }


def cmul(left, right):
    highest = lax.Precision.HIGHEST
    left_re, left_im = left[..., 0, :, :], left[..., 1, :, :]
    right_re, right_im = right[..., 0, :, :], right[..., 1, :, :]
    real_part = jnp.matmul(left_re, right_re, precision=highest) - jnp.matmul(left_im, right_im, precision=highest)
    imag_part = jnp.matmul(left_re, right_im, precision=highest) + jnp.matmul(left_im, right_re, precision=highest)
    return jnp.stack([real_part, imag_part], axis=-3)


def invert(intersection, eye_c):
    estimate = eye_c
    for newton_step in range(NEWTON):
        estimate = cmul(estimate, 2.0 * eye_c - cmul(intersection, estimate))
    return estimate


def project(proj_table, columns, swapped):
    real_part = jnp.dot(proj_table.T, columns, preferred_element_type=jnp.float32)
    imag_part = jnp.dot(proj_table.T, swapped, preferred_element_type=jnp.float32)
    return jnp.stack([real_part, imag_part])


def reference(coeffs, projectors, proj_deriv, shift_map, atom_of):
    proj_table = projectors.reshape(2 * NG, NP)
    deriv_table = proj_deriv.reshape(2 * NG, NP)
    eye_c = jnp.stack([jnp.eye(NB, dtype=jnp.float32), jnp.zeros((NB, NB), jnp.float32)])

    def k_point(state_pair, k_index):
        running, accumulated = state_pair
        own_point = lax.dynamic_index_in_dim(coeffs, k_index, 0, keepdims=False)
        following = lax.dynamic_index_in_dim(coeffs, (k_index + 1) % NK, 0, keepdims=False)
        following = jnp.where(k_index == NK - 1, following[:, shift_map, :], following)
        columns = own_point.reshape(2 * NG, NB)
        own_swap = jnp.concatenate([own_point[1], -own_point[0]], axis=0)
        next_cols = following.reshape(2 * NG, NB)
        next_swap = jnp.concatenate([following[1], -following[0]], axis=0)
        intersections = jnp.stack([
            jnp.dot(columns.T, next_cols, preferred_element_type=jnp.float32),
            jnp.dot(columns.T, next_swap, preferred_element_type=jnp.float32)])
        inverse = invert(intersections, eye_c)
        running = cmul(running, inverse)
        proj_vals = project(proj_table, columns, own_swap)
        deriv_vals = project(deriv_table, columns, own_swap)
        weighted = cmul(proj_vals, running)
        accumulated = accumulated + jnp.sum(deriv_vals[0] * weighted[1] - deriv_vals[1] * weighted[0], axis=1)
        return (running, accumulated), running

    (running, accumulated), transport = lax.scan(
        k_point, (eye_c, jnp.zeros((NP,), jnp.float32)), jnp.arange(NK, dtype=jnp.int32))
    onehot = (atom_of[None, :] == jnp.arange(NA, dtype=jnp.int32)[:, None]).astype(jnp.float32)
    forces = jnp.dot(onehot, accumulated / NK, precision=lax.Precision.HIGHEST)
    return transport, forces
```

```python
import jax
import jax.numpy as jnp
from jax import lax
from jax.sharding import PartitionSpec as P

NA = 128
NEWTON = 2
HI = lax.Precision.HIGHEST


def shifted(block, axis, distance):
    n = lax.axis_size(axis)
    return lax.ppermute(block, axis, [(i, (i + distance) % n) for i in range(n)])


def swapped(block, axis, bit):
    n = lax.axis_size(axis)
    return lax.ppermute(block, axis, [(i, i ^ bit) for i in range(n)])


def cmul(left, right):
    lr, li = left[0], left[1]
    rr, ri = right[0], right[1]
    mm = lambda a, b: jnp.matmul(a, b, precision=HI)
    return jnp.stack([mm(lr, rr) - mm(li, ri), mm(lr, ri) + mm(li, rr)])


def invert(matrix, eye_c):
    estimate = 2.0 * eye_c - matrix
    for _ in range(NEWTON - 1):
        estimate = cmul(estimate, 2.0 * eye_c - cmul(matrix, estimate))
    return estimate


def encode(values):
    top = jnp.maximum(jnp.max(jnp.abs(values), axis=1, keepdims=True), 1e-30)
    power = jnp.floor(jnp.log2(top)) + 1.0
    codes = jnp.clip(jnp.round(values * jnp.exp2(15.0 - power)), -32767.0, 32767.0)
    powers = jnp.broadcast_to(power, (values.shape[0], 16, values.shape[2]))
    return jnp.concatenate([codes, powers], axis=1).astype(jnp.int16)


def decode(coded):
    rows = coded.shape[1] - 16
    power = coded[:, rows : rows + 1].astype(jnp.float32)
    return coded[:, :rows].astype(jnp.float32) * jnp.exp2(power - 15.0)


def scatter_codes(values, me, size):
    share = values.shape[2] // size
    cut = lambda a, who: lax.dynamic_slice_in_dim(a, who * share, share, 2)
    total = cut(values, me)
    coded = encode(values)
    for s in range(1, size):
        total = total + decode(shifted(cut(coded, (me + s) % size), "ga", s))
    return total


def local(coeffs, projectors, proj_deriv, shift_map, atom_of):
    points, _, rows, bands = coeffs.shape
    n_proj = projectors.shape[2]
    n_ka = lax.axis_size("ka")
    n_ga = lax.axis_size("ga")
    position = lax.axis_index("ka")
    layer = lax.axis_index("ga")
    eye_c = jnp.stack([jnp.eye(bands, dtype=jnp.float32), jnp.zeros((bands, bands), jnp.float32)])
    arrived = shifted(coeffs[0], "ka", -1)

    columns = coeffs.reshape(points, 2 * rows, bands)
    own_swap = jnp.concatenate([coeffs[:, 1], -coeffs[:, 0]], axis=1)
    both = jnp.concatenate([columns, own_swap], axis=2)

    def project(table):
        flat = table.reshape(2 * rows, n_proj)
        return jnp.einsum("kgn,gp->knp", both, flat, preferred_element_type=jnp.float32)

    b_vals = scatter_codes(project(projectors), layer, n_ga)
    d_part = project(proj_deriv)

    place = shift_map % rows
    last = coeffs[points - 1]

    def unmap():
        onehot = (place[:, None] == jnp.arange(rows, dtype=jnp.int32)[None, :]).astype(jnp.bfloat16)
        return jnp.einsum("gh,cgn->chn", onehot, last, preferred_element_type=jnp.float32).astype(jnp.bfloat16)

    last = lax.cond(position == n_ka - 1, unmap, lambda: last)

    def overlap(mine, theirs):
        a = mine.reshape(2 * rows, bands)
        t = theirs.reshape(2 * rows, bands)
        ts = jnp.concatenate([theirs[1], -theirs[0]], axis=0)
        mm = lambda x, y: lax.dot_general(x, y, (((0,), (0,)), ((), ())), preferred_element_type=jnp.float32)
        return jnp.stack([mm(a, t), mm(a, ts)])

    parts = [overlap(coeffs[i], coeffs[i + 1]) for i in range(points - 1)] + [overlap(last, arrived)]
    part = jnp.stack(parts)
    share = bands // n_ga
    cut = lambda a, who: lax.dynamic_slice_in_dim(a, who * share, share, 2)
    mine = cut(part, layer)
    for s in range(1, n_ga):
        mine = mine + shifted(cut(part, (layer + s) % n_ga), "ga", s)
    whole = jnp.zeros(part.shape, jnp.float32)
    whole = lax.dynamic_update_slice_in_dim(whole, mine, layer * share, 2)
    for s in range(1, n_ga):
        whole = lax.dynamic_update_slice_in_dim(whole, shifted(mine, "ga", s), ((layer - s) % n_ga) * share, 2)

    whole, d_part = lax.optimization_barrier((whole, d_part))
    d_vals = scatter_codes(d_part, layer, n_ga)

    inverses = [invert(whole[i], eye_c) for i in range(points)]
    chain = [inverses[0]]
    for i in range(1, points):
        chain.append(cmul(chain[-1], inverses[i]))

    odd = position % 2 == 1
    partner = swapped(chain[-1], "ka", 1)
    pair = cmul(jnp.where(odd, partner, chain[-1]), jnp.where(odd, chain[-1], partner))
    half = bands // 2
    cut_half = lambda a, who: lax.dynamic_slice_in_dim(a, who * half, half, 1)
    my_half = cut_half(pair, position % 2)
    halves = jnp.stack([shifted(my_half, "ka", 2 * s) for s in range(1, n_ka // 2)])
    others = swapped(halves, "ka", 1)
    before = None
    for s in range(1, n_ka // 2):
        a, b = halves[s - 1], others[s - 1]
        block = jnp.concatenate([jnp.where(odd, b, a), jnp.where(odd, a, b)], axis=1)
        block = jnp.where(position // 2 >= s, block, eye_c)
        before = block if before is None else cmul(block, before)
    if points == 1:
        transports = [cmul(before, jnp.where(odd, pair, chain[0]))]
    else:
        before = cmul(before, jnp.where(odd, partner, eye_c))
        transports = [cmul(before, link) for link in chain]

    total = jnp.zeros((n_proj // n_ga,), jnp.float32)
    tmm = lambda x, y: lax.dot_general(x, y, (((0,), (0,)), ((), ())), precision=HI)
    for i in range(points):
        tr, ti = transports[i][0], transports[i][1]
        br, bi = b_vals[i, :bands], b_vals[i, bands:]
        dr, di = d_vals[i, :bands], d_vals[i, bands:]
        wr = tmm(tr, br) - tmm(ti, bi)
        wi = tmm(tr, bi) + tmm(ti, br)
        total = total + jnp.sum(dr * wi - di * wr, axis=0)
    total = total / (points * n_ka)
    width = n_proj // n_ga
    owners = lax.dynamic_slice_in_dim(atom_of, layer * width, width, 0)
    onehot = (owners[:, None] == jnp.arange(NA, dtype=jnp.int32)[None, :]).astype(jnp.float32)
    forces = jnp.dot(total[None, :], onehot, precision=HI)
    for axis, n in (("ka", n_ka), ("ga", n_ga)):
        bit = 1
        while bit < n:
            forces = forces + swapped(forces, axis, bit)
            bit *= 2
    return jnp.stack(transports), forces[0]


def solution(mesh):
    placed = (P("ka", None, "ga", None), P(None, "ga", None), P(None, "ga", None), P("ga"), P())
    return jax.shard_map(
        local,
        mesh=mesh,
        in_specs=placed,
        out_specs=(P("ka", None, None, None), P()),
        check_vma=False,
    )
```
